512 devices in a mesh: row: 32 (over y, x), col: 16 (over z, core).
Axes of the slice: x: 4, y: 8, z: 8, core: 2. Of those that a mesh axis runs over, the one named last changes fastest.
Arguments:
- pair_factors: float32 [12288, 1024], P(('row', 'col')), may hold values from -0.09375 to 0.09375
- k_prev: float32 [12288, 12288], P('row', 'col'), as said below
- energies: float32 [12288], P('row'), may hold values from 0.3 to 2
Outputs:
- casida: float32 [12288, 12288], P('row', 'col')
- vectors: float32 [12288, 8], P('row')
- images: float32 [12288, 8], P('row')
- tridiagonal: float32 [2, 8], replicated
The draws below stay inside these ranges and needn't reach their ends.
Inputs may be any that keep to these rules, and one draw needn't show every extreme that they name: k_prev is exactly symmetric.
All inputs are finite; a program needn't handle non-finite values.
Results may differ from the reference program's by a relative error of at most 0.0003.
Values sent between devices are 32-bit elements; how exact they have to be, the bound alone decides.
A program may use at most 64 MiB of HBM per device.

```python
import math
import jax
import jax.numpy as jnp
from jax import lax

N = 12288
PC = 8
AUXW = 1024


def draw_k_prev(key, part):
    base = 0.02 * jax.random.normal(key, (N, N), jnp.float32)
    return (base + base.T) * 0.7071


def shard_levels(key, extent, split, low, largest):
    factor_of, own = 1.0, jax.random.fold_in(key, 6)
    for position, shards_of in split:
        heights = jnp.exp(jax.random.uniform(jax.random.fold_in(own, position), (shards_of,), jnp.float32, low / len(split), largest / len(split)))
        factor_of = factor_of * jnp.repeat(heights, extent[position] // shards_of).reshape([-1 if axis == position else 1 for axis in range(len(extent))])
    return factor_of


def scatter_about(stream_key, shape, spread, limit, cuts=(), kind=jnp.bfloat16):
    drawn = jax.random.normal(stream_key, shape, jnp.float32) * spread
    if len(cuts) > 0:
        drawn = shard_levels(stream_key, shape, cuts, -0.22, 0.18) * drawn
    return jnp.clip(drawn, min=-limit, max=limit).astype(kind)


def setup_inputs(seed: int = 0) -> dict:
    seeds = jax.random.split(jax.random.key(seed), 4)
    pair_factors = scatter_about(seeds[0], (N, AUXW), (0.5 * AUXW ** -0.5), 0.09375, ((0, 512),), jnp.float32)
    k_prev = draw_k_prev(jax.random.fold_in(seeds[3], 71), 0)
    energies = jnp.clip(jnp.exp(math.log(2.0) - 1.89712 * jax.random.uniform(seeds[2], (N,), jnp.float32) ** shard_levels(seeds[2], (N,), ((0, 32),), -0.2, 0.2)), 0.3, 2.0)
    return {"pair_factors": pair_factors, "k_prev": k_prev, "energies": energies}


def reference(pair_factors, k_prev, energies):
    coupling = k_prev + jnp.dot(pair_factors, pair_factors.T, precision=lax.Precision.HIGHEST, preferred_element_type=jnp.float32)
    casida = 4.0 * coupling + jnp.diag(energies)
    row_ids = jnp.arange(N, dtype=jnp.int32)
    col_ids = jnp.arange(PC, dtype=jnp.int32)
    upper = jnp.zeros((N, PC), jnp.float32)
    lower = jnp.zeros((N, PC), jnp.float32)
    diag_list = []
    sub_list = []
    for column_at in range(PC):
        column = casida[:, column_at] - jnp.dot(upper, lower[column_at], precision=lax.Precision.HIGHEST) - jnp.dot(lower, upper[column_at], precision=lax.Precision.HIGHEST)
        diag_list.append(column[column_at])
        below = jnp.where(row_ids > column_at, column, 0.0)
        lead = column[column_at + 1]
        sigma = jnp.sum(below * below)
        root = jnp.sqrt(sigma)
        alpha = jnp.where(lead >= 0, -root, root)
        vector = below - alpha * (row_ids == column_at + 1).astype(jnp.float32)
        length = jnp.sqrt(jnp.maximum(2.0 * (sigma + jnp.abs(lead) * root), 1.0))
        unit = vector / length
        image = jnp.dot(casida, unit, precision=lax.Precision.HIGHEST)
        image = image - jnp.dot(upper, jnp.dot(lower.T, unit, precision=lax.Precision.HIGHEST), precision=lax.Precision.HIGHEST)
        image = image - jnp.dot(lower, jnp.dot(upper.T, unit, precision=lax.Precision.HIGHEST), precision=lax.Precision.HIGHEST)
        image = 2.0 * image
        partner = image - jnp.sum(image * unit) * unit
        pick = (col_ids == column_at).astype(jnp.float32)[None, :]
        upper = upper + unit[:, None] * pick
        lower = lower + partner[:, None] * pick
        sub_list.append(alpha)
    scale = jnp.sqrt(jnp.float32(N))
    tridiagonal = jnp.stack([jnp.stack(diag_list), jnp.stack(sub_list)])
    return (casida, scale * upper, scale * lower, tridiagonal)
```

```python
import functools

import jax
import jax.numpy as jnp
from jax import lax
from jax.experimental import pallas as pl
from jax.experimental.pallas import tpu as pltpu
from jax.sharding import PartitionSpec as P

N = 12288
PC = 8
AUX = 1024
CH = 24
ROWS = 384
COLS = 768
MESH = pl.DeviceIdType.MESH
HI = lax.Precision.HIGHEST


def chunk(slot):
    return pl.ds(pl.multiple_of(slot * CH, 8), CH)


def remote(src, dst, send, recv, row, col):
    return pltpu.make_async_remote_copy(
        src_ref=src, dst_ref=dst, send_sem=send, recv_sem=recv,
        device_id=(row, col), device_id_type=MESH,
    )


def iota(shape, axis):
    return lax.broadcasted_iota(jnp.int32, shape, axis)


def lane_sum(a):
    width = a.shape[1] // 128
    total = a[:, 0:128]
    for t in range(1, width):
        total = total + a[:, 128 * t : 128 * (t + 1)]
    return total


def kernel(
    pf, kp_hbm, en, casida, uw, tri,
    left, right, kp, a, ae, v, zbuf, xbuf, tbuf, abuf, spare,
    local, ls, lr, rs, rr, zs, zr, xs, xr, ts, tr, bs, br,
):
    r = lax.axis_index("row")
    c = lax.axis_index("col")
    y, x = r // 4, r % 4
    z, k = c // 2, c % 2

    kp_in = pltpu.make_async_copy(kp_hbm, kp, local.at[0])
    kp_in.start()
    own_in = pltpu.make_async_copy(pf, left.at[chunk(c)], local.at[1])
    own_in.start()

    barrier = pltpu.get_barrier_semaphore()

    def greet_row(d, _):
        pl.semaphore_signal(barrier, inc=1, device_id=((r + d) % 32, c), device_id_type=MESH)
        return 0

    def greet_col(d, _):
        pl.semaphore_signal(barrier, inc=1, device_id=(r, (c + d) % 16), device_id_type=MESH)
        return 0

    lax.fori_loop(1, 32, greet_row, 0)
    lax.fori_loop(1, 16, greet_col, 0)
    v[...] = jnp.zeros_like(v)
    pl.semaphore_wait(barrier, 46)
    own_in.wait()

    def l_copy(slot, direction):
        if direction == 0:
            col = (z + 1) % 8 * 2 + k
        elif direction == 1:
            col = (z + 7) % 8 * 2 + k
        else:
            col = 2 * z + (1 - k)
        return remote(left.at[chunk(slot)], left.at[chunk(slot)], ls.at[direction, slot], lr.at[slot], r, col)

    def l_wait(slot):
        pltpu.make_async_copy(left.at[chunk(slot)], left.at[chunk(slot)], lr.at[slot]).wait()

    def stage_slots(i, core):
        return (z + 8 - i) % 8 * 2 + core, (z + i) % 8 * 2 + core

    def r_rows(b, slot):
        return pl.ds(pl.multiple_of(b * ROWS + slot * CH, 8), CH)

    def r_copy(b, slot, direction, from_left):
        row = (
            (y + 1) % 8 * 4 + x,
            (y + 7) % 8 * 4 + x,
            y * 4 + (x + 1) % 4,
            y * 4 + (x + 3) % 4,
        )[direction]
        src = left.at[chunk(slot)] if from_left else right.at[r_rows(b, slot)]
        return remote(src, right.at[r_rows(b, slot)], rs.at[direction, b, slot], rr.at[b, slot], row, c)

    dy = (y - z + 8) % 8
    ydist = jnp.where(dy <= 4, dy, 8 - dy)
    groups = []
    for b in range(2):
        dx = (x - (2 * k + b) + 4) % 4
        xdist = jnp.where(dx <= 2, dx, 1)
        groups.append((b, dx, ydist + xdist))

    def r_roles(b, dx, slot, even):
        at_source = (dx == 0) & (dy == 0)
        column = dx == 0
        yield 0, True, at_source
        yield 1, True, at_source
        yield 0, False, column & (dy >= 1) & (dy <= 3)
        yield 1, False, column & (dy >= 6)
        yield 2, True, at_source
        yield 3, True, at_source
        yield 2, False, (column & (dy > 0)) | ((dx == 1) & even)
        yield 3, False, (column & (dy > 0)) | ((dx == 3) & (not even))

    def local_copy(b, slot):
        return pltpu.make_async_copy(left.at[chunk(slot)], right.at[r_rows(b, slot)], rr.at[b, slot])

    def r_process(b, dx, slot, even):
        at_source = (dx == 0) & (dy == 0)

        @pl.when(at_source)
        def _():
            local_copy(b, slot).start()

        @pl.when(jnp.logical_not(at_source))
        def _():
            pltpu.make_async_copy(right.at[r_rows(b, slot)], right.at[r_rows(b, slot)], rr.at[b, slot]).wait()

        for direction, from_left, cond in r_roles(b, dx, slot, even):
            @pl.when(cond)
            def _(direction=direction, from_left=from_left):
                r_copy(b, slot, direction, from_left).start()

    def r_stage(t, core_same):
        core = k if core_same else 1 - k
        for b, dx, dist in groups:
            i = t - dist
            @pl.when((i >= 0) & (i <= 4))
            def _(b=b, dx=dx, i=i):
                minus, plus = stage_slots(i, core)
                r_process(b, dx, minus, core_same)
                @pl.when((i >= 1) & (i <= 3))
                def _():
                    r_process(b, dx, plus, core_same)

    def gather_step(t, _):
        @pl.when(t == 0)
        def _():
            for direction in range(3):
                l_copy(c, direction).start()

        @pl.when((t >= 1) & (t <= 4))
        def _():
            minus, plus = stage_slots(t, k)
            l_wait(minus)
            @pl.when(t < 4)
            def _():
                l_copy(minus, 0).start()
            l_copy(minus, 2).start()
            @pl.when(t < 4)
            def _():
                l_wait(plus)
                @pl.when(t < 3)
                def _():
                    l_copy(plus, 1).start()
                l_copy(plus, 2).start()

        r_stage(t, True)

        @pl.when(t <= 4)
        def _():
            minus, plus = stage_slots(t, 1 - k)
            l_wait(minus)
            @pl.when((t >= 1) & (t <= 3))
            def _():
                l_wait(plus)

        r_stage(t, False)
        return 0

    lax.fori_loop(0, 11, gather_step, 0)

    def l_drain(slot, _):
        dz = (slot // 2 - z + 8) % 8
        mine = slot % 2 == k
        @pl.when(mine & ((dz == 0) | (dz >= 5)))
        def _():
            l_copy(slot, 0).wait_send()
        @pl.when(mine & (dz <= 2))
        def _():
            l_copy(slot, 1).wait_send()
        @pl.when(mine)
        def _():
            l_copy(slot, 2).wait_send()
        for b, dx, _d in groups:
            at_source = (dx == 0) & (dy == 0)
            @pl.when(at_source)
            def _(b=b):
                local_copy(b, slot).wait()
            for same in (True, False):
                @pl.when(mine if same else jnp.logical_not(mine))
                def _(b=b, dx=dx, same=same):
                    for direction, from_left, cond in r_roles(b, dx, slot, same):
                        @pl.when(cond)
                        def _(direction=direction, from_left=from_left):
                            r_copy(b, slot, direction, from_left).wait_send()
        return 0

    lax.fori_loop(0, 16, l_drain, 0)
    kp_in.wait()

    def block(t, _):
        at = pl.ds(pl.multiple_of(t * 128, 128), 128)
        prod = lax.dot_general(
            left[...], right[at, :], (((1,), (1,)), ((), ())),
            precision=HI, preferred_element_type=jnp.float32,
        )
        a[:, at] = 4.0 * (kp[:, at] + prod)
        return 0

    lax.fori_loop(0, 6, block, 0)
    eye = iota((ROWS, ROWS), 0) == iota((ROWS, ROWS), 1)
    for b in range(2):
        @pl.when(r == 2 * c + b)
        def _(b=b):
            at = slice(b * ROWS, (b + 1) * ROWS)
            a[:, at] = a[:, at] + jnp.where(eye, en[...], 0.0)
    out = pltpu.make_async_copy(a, casida, local.at[0])
    out.start()

    def peers_row(send):
        def body(d, _):
            send((r + d) % 32, c)
            return 0
        lax.fori_loop(1, 32, body, 0)

    def peers_col(send):
        def body(d, _):
            send(r, (c + d) % 16)
            return 0
        lax.fori_loop(1, 16, body, 0)

    def ae_copy(row, col):
        return remote(ae, ae, bs.at[0], br.at[0], row, col)

    def a0_copy(row, col):
        return remote(abuf, abuf, bs.at[1], br.at[1], row, col)

    @pl.when(c == 0)
    def _():
        head = a[:, 0:128].T
        for i in range(PC + 1):
            ae[i] = head[i : i + 1, :]
        peers_col(lambda row, col: ae_copy(row, col).start())

    @pl.when(r == 0)
    def _():
        abuf[...] = a[0:1, :]
        peers_row(lambda row, col: a0_copy(row, col).start())

    @pl.when(c != 0)
    def _():
        ae_copy(r, c).wait_recv()

    @pl.when(r != 0)
    def _():
        a0_copy(r, c).wait_recv()

    lane = iota((1, 128), 1)
    row_ids = r * ROWS + iota((1, ROWS), 1)
    col_ids = c * COLS + iota((1, COLS), 1)
    sub24 = iota((24, 128), 0)
    lane24 = iota((24, 128), 1)

    def column_of(row_form, shift):
        return jnp.sum(jnp.where(lane24 == sub24 + shift, row_form, 0.0), axis=1, keepdims=True)

    def zdrain(sem, ref, count):
        pltpu.make_async_copy(ref.at[pl.ds(0, count)], ref.at[pl.ds(0, count)], sem).wait()

    full_c = abuf[...]
    full_r = ae[0]
    heads = jnp.zeros((24, 128), jnp.float32)
    dots = jnp.zeros((24, 1), jnp.float32)
    diag = jnp.zeros((1, 128), jnp.float32)
    sub = jnp.zeros((1, 128), jnp.float32)
    for j in range(PC):
        xc = jnp.where(col_ids > j, full_c, 0.0)
        xrow = jnp.where(row_ids > j, full_r, 0.0)
        acc = a[:, 0:128] * xc[:, 0:128]
        for t in range(1, 6):
            acc = acc + a[:, 128 * t : 128 * (t + 1)] * xc[:, 128 * t : 128 * (t + 1)]
        part = lax.dot_general(
            jnp.ones((8, 128), jnp.float32), acc, (((1,), (1,)), ((), ())),
            precision=HI, preferred_element_type=jnp.float32,
        )[0:1, :]
        sq = lane_sum(xc * xc)
        sq = sq + pltpu.roll(sq, 64, 1)
        side = jnp.where(lane >= 64, sq, jnp.where((lane < 16) & (c == 0), full_c[:, 0:128], 0.0))
        zbuf[j, c] = jnp.concatenate([part, side], axis=1)
        peers_col(lambda row, col: remote(zbuf.at[j, c], zbuf.at[j, c], zs.at[j], zr.at[j], row, col).start())
        zdrain(zr.at[j], zbuf.at[j], 15)
        tot = zbuf[j, 0]
        for s in range(1, 16):
            tot = tot + zbuf[j, s]
        side = tot[:, ROWS:]
        head_full = jnp.where(lane < 16, side, 0.0)
        hx = jnp.where(lane > j, head_full, 0.0)
        sigma = jnp.sum(jnp.where(lane >= 64, side, 0.0), axis=1, keepdims=True)
        lead = hx[:, j + 1 : j + 2]
        root = jnp.sqrt(sigma)
        alpha = jnp.where(lead >= 0, -root, root)
        length = jnp.sqrt(jnp.maximum(2.0 * (sigma + jnp.abs(lead) * root), 1.0))
        inv = 1.0 / length
        diag = jnp.where(lane == j, head_full[:, j : j + 1], diag)
        sub = jnp.where(lane == j, alpha, sub)
        uc = (xc - jnp.where(col_ids == j + 1, alpha, 0.0)) * inv
        ur = (xrow - jnp.where(row_ids == j + 1, alpha, 0.0)) * inv
        hu = (hx - jnp.where(lane == j + 1, alpha, 0.0)) * inv
        top = hu[:, j + 1 : j + 2]
        aej = ae[j + 1]
        au = (tot[:, :ROWS] - alpha * aej) * inv
        vv = v[...]
        hcol = heads[:, j + 1 : j + 2]
        coef = (dots - alpha * hcol) * inv
        swap_coef = jnp.concatenate([coef[8:16], coef[0:8]], axis=0)
        swap_head = jnp.concatenate([hcol[8:16], hcol[0:8]], axis=0)
        p = 2.0 * (au - jnp.sum(vv[0:16] * swap_coef, axis=0, keepdims=True))
        cand = aej - jnp.sum(vv[0:16] * swap_head, axis=0, keepdims=True) - top * p
        v[j : j + 1, :] = ur
        v[16:17, :] = p
        vv = v[...]
        below = row_ids > j + 1
        sm = jnp.where(below, cand, 0.0)
        um = jnp.where(below, ur, 0.0)
        ds_ = jnp.sum(lane_sum(vv * sm), axis=1, keepdims=True)
        dm_ = jnp.sum(lane_sum(vv * um), axis=1, keepdims=True)
        row = jnp.sum(
            jnp.where(lane24 == sub24, ds_, 0.0) + jnp.where(lane24 == sub24 + 32, dm_, 0.0),
            axis=0, keepdims=True,
        )
        ph = jnp.where((lane < 16) & (r == 0), p[:, 0:128], 0.0)
        xbuf[j, r] = row + pltpu.roll(ph, 64, 1)
        peers_row(lambda row_, col: remote(xbuf.at[j, r], xbuf.at[j, r], xs.at[j], xr.at[j], row_, col).start())

        def t_copy(b, row_, col):
            return remote(tbuf.at[j, b], tbuf.at[j, b], ts.at[j], tr.at[j, b], row_, col)

        if j + 1 < PC:
            for b in range(2):
                @pl.when(r == 2 * c + b)
                def _(b=b):
                    tbuf[j, b] = cand
                    peers_row(lambda row_, col: t_copy(b, row_, col).start())
        zdrain(xr.at[j], xbuf.at[j], 31)
        sums = xbuf[j, 0]
        for s in range(1, 32):
            sums = sums + xbuf[j, s]
        hp = jnp.where(lane < 16, pltpu.roll(sums, 64, 1), 0.0)
        dsc = column_of(sums, 0)
        dmc = column_of(sums, 32)
        ptop = hp[:, j + 1 : j + 2]
        kappa = dmc[16:17] + ptop * top
        beta = 2.0 * kappa * top - ptop
        w = p - kappa * ur
        hw = hp - kappa * hu
        v[8 + j : 9 + j, :] = w
        heads = jnp.where(sub24 == j, hu, jnp.where(sub24 == 8 + j, hw, heads))
        if j + 1 < PC:
            for b in range(2):
                @pl.when(r != 2 * c + b)
                def _(b=b):
                    t_copy(b, r, c).wait_recv()
            full_c = jnp.concatenate([tbuf[j, 0], tbuf[j, 1]], axis=1) + beta * uc
            full_r = cand + beta * ur
            dots = dsc + beta * dmc
            wdot = dots[16:17] - kappa * dots[j : j + 1]
            dots = jnp.where(iota((24, 1), 0) == 8 + j, wdot, dots)

    uw[...] = v[0:16, :]
    tri[...] = jnp.concatenate([diag, sub], axis=0)

    for j in range(PC):
        zdrain(zs.at[j], zbuf.at[j], 15)
        zdrain(xs.at[j], xbuf.at[j], 31)
        if j + 1 < PC:
            @pl.when(r // 2 == c)
            def _(j=j):
                zdrain(ts.at[j], spare, 31)

    @pl.when(c == 0)
    def _():
        zdrain(bs.at[0], spare, 15 * (PC + 1))

    @pl.when(r == 0)
    def _():
        zdrain(bs.at[1], spare, 31 * 2)

    out.wait()


def solution(mesh):
    f32 = jnp.float32
    vmem = pl.BlockSpec(memory_space=pltpu.VMEM)
    hbm = pl.BlockSpec(memory_space=pl.ANY)
    dma = pltpu.SemaphoreType.DMA

    def shards(pair_factors, k_prev, energies):
        casida, uw, tri = pl.pallas_call(
            kernel,
            out_shape=(
                jax.ShapeDtypeStruct((ROWS, COLS), f32),
                jax.ShapeDtypeStruct((2 * PC, ROWS), f32),
                jax.ShapeDtypeStruct((2, 128), f32),
            ),
            in_specs=[hbm, hbm, vmem],
            out_specs=(hbm, vmem, vmem),
            scratch_shapes=[
                pltpu.VMEM((ROWS, AUX), f32),
                pltpu.VMEM((COLS, AUX), f32),
                pltpu.VMEM((ROWS, COLS), f32),
                pltpu.VMEM((ROWS, COLS), f32),
                pltpu.VMEM((PC + 1, 1, ROWS), f32),
                pltpu.VMEM((24, ROWS), f32),
                pltpu.VMEM((PC, 16, 1, ROWS + 128), f32),
                pltpu.VMEM((PC, 32, 1, 128), f32),
                pltpu.VMEM((PC, 2, 1, ROWS), f32),
                pltpu.VMEM((1, COLS), f32),
                pltpu.VMEM((15 * (PC + 1), 1, ROWS), f32),
                dma((2,)),
                dma((3, 16)), dma((16,)), dma((4, 2, 16)), dma((2, 16)),
                dma((PC,)), dma((PC,)), dma((PC,)), dma((PC,)),
                dma((PC,)), dma((PC, 2)), dma((2,)), dma((2,)),
            ],
            compiler_params=pltpu.CompilerParams(collective_id=0, has_side_effects=True),
            name="casida",
        )(pair_factors, k_prev, energies.reshape(1, ROWS))
        scale = jnp.sqrt(f32(N))
        return casida, scale * uw[:PC].T, scale * uw[PC:].T, tri[:, :PC]

    return jax.shard_map(
        shards, mesh=mesh,
        in_specs=(P(("row", "col"), None), P("row", "col"), P("row")),
        out_specs=(P("row", "col"), P("row", None), P("row", None), P()),
        check_vma=False,
    )
```
